32 devices in a mesh: grp: 4 (over z), fsdp: 4 (over y, x), tp: 2 (over core).
Axes of the slice: x: 2, y: 2, z: 4, core: 2. Of those that a mesh axis runs over, the one named last changes fastest.
Arguments:
- frames: bfloat16 [768, 5120], P('fsdp', 'grp'), may hold values from -6 to 6
- projector: bfloat16 [5120, 8192], P('grp', 'tp'), may hold values from -0.078125 to 0.078125
- text_token_embedding: bfloat16 [4096, 8192], P(('grp', 'fsdp'), 'tp'), may hold values from -6 to 6
- norm_gain_vector: float32 [8192], replicated, may hold values from 0.1 to 1.9
- frozen: bfloat16 [8192, 1024], P('fsdp', 'tp'), may hold values from -0.0625 to 0.0625
- adapter_down_map: bfloat16 [8192, 64], P('fsdp'), may hold values from -0.0625 to 0.0625
- adapter_up_map: bfloat16 [64, 1024], P(None, 'tp'), may hold values from -0.75 to 0.75
- clip_frame_length: int32 [4, 4, 4], P('fsdp'), may hold values from 1 to 24, as said below
- audio_first_token: int32 [4, 4, 4], P('fsdp'), may hold values from 0 to 255, as said below
- segment_document_index: int32 [4096], P(('grp', 'fsdp')), may hold values from 0 to 63, never falling along the last dimension, each value on 1 to 256 neighbouring positions
- keep_document_flags: int32 [64], replicated, may hold values 0 or 1
- cotangent: bfloat16 [4096, 1024], P(('grp', 'fsdp'), 'tp'), may hold values from -0.09375 to 0.09375
Outputs:
- value_output: bfloat16 [4096, 1024], P(('grp', 'fsdp'), 'tp')
- projector_grad: float32 [5120, 8192], P('grp', 'tp')
- down_map_gradient: float32 [8192, 64], P('tp')
- up_map_gradient: float32 [64, 1024], P(None, 'tp')
The draws below stay inside these ranges and needn't reach their ends.
Inputs may be any that keep to these rules, and one draw needn't show every extreme that they name: `clip_frame_length`: entry [f, g, k] is the length of clip k of frame block f * 4 + g; the 4 clips of a block sum to 48, and one of them has exactly 24 frames. `audio_first_token`: entry [f, g, k] is the first token, among the 256 tokens of block k * 4 + f, of the audio slots of clip k of frame block f * 4 + g; the 4 clips that one token block takes lie in distinct aligned windows of 64 tokens.
All inputs are finite; a program needn't handle non-finite values.
Results may differ from the reference program's by a relative error of at most 0.018.
Values may be sent and summed in bfloat16 or wider, within the bound.
A program may use at most 128 MiB of HBM per device.

```python
import math
import jax
import jax.numpy as jnp
import numpy as np
from jax import lax

MODEL_WIDTH = 8192
VALUE_WIDTH = 1024
DA = 5120
ADAPTER_RANK = 64
TOK_DEV = 256
FRAMES_DEV = 48
CAP = 24
WIN = 64
TOKENS = 4096
FRAMES = 768
DOCS = 64
N_GRP = 4
N_FSDP = 4
N_TP = 2


def clip_layout(key):
    base_key = jax.random.fold_in(key, 7321)
    key_order, key_shift, key_window, key_offset = jax.random.split(base_key, 4)
    rows_total = N_FSDP * N_GRP
    half_cap = CAP // 2
    pair_count = (N_GRP - 3) // 2
    scores = jax.random.randint(key_order, (rows_total, N_GRP), 0, 1 << 20) * N_GRP + lax.broadcasted_iota(jnp.int32, (rows_total, N_GRP), 1)
    ranking = jnp.argsort(scores, axis=1, stable=True).astype(jnp.int32)
    deltas = jax.random.randint(key_shift, (rows_total, pair_count), -(half_cap - 1), half_cap)
    adjust = jnp.zeros((rows_total, N_GRP), jnp.int32)
    adjust = adjust.at[:, 0].set(half_cap)
    adjust = adjust.at[:, 1].set(-(half_cap // 2))
    adjust = adjust.at[:, 2].set(-(half_cap - half_cap // 2))
    adjust = adjust.at[:, 3:3 + 2 * pair_count:2].set(deltas)
    adjust = adjust.at[:, 4:4 + 2 * pair_count:2].set(-deltas)
    by_rank = half_cap + adjust
    inverse = jnp.argsort(ranking, axis=1, stable=True).astype(jnp.int32)
    clip_sizes = jnp.take_along_axis(by_rank, inverse, axis=1).reshape(N_FSDP, N_GRP, N_GRP)
    window_scores = jax.random.randint(key_window, (N_FSDP, N_GRP, N_GRP), 0, 1 << 20) * N_GRP + lax.broadcasted_iota(jnp.int32, (N_FSDP, N_GRP, N_GRP), 1)
    window = jnp.argsort(window_scores, axis=1, stable=True).astype(jnp.int32)
    free_room = WIN - clip_sizes + 1
    offsets = jax.random.randint(key_offset, (N_FSDP, N_GRP, N_GRP), 0, free_room)
    positions = window * WIN + offsets
    return (clip_sizes.astype(jnp.int32), positions.astype(jnp.int32))


def draw_clip_frame_length(key, part):
    return clip_layout(key)[0]


def draw_audio_first_token(key, part):
    return clip_layout(key)[1]


def touch_ends(values, key, smallest, largest):
    longest = values.shape.index(max(values.shape))
    spots = []
    for shift in (0, 1):
        where = [jax.random.randint(jax.random.fold_in(key, axis), (), 0, length) for axis, length in enumerate(values.shape)]
        where[longest] = (where[longest] + shift) % values.shape[longest]
        spots.append(tuple(where))
    return values.at[spots[0]].set(smallest).at[spots[1]].set(largest)


def block_scale(rng, dims, cuts, low, high):
    level = 1.0
    for dim, parts in cuts:
        heights = jax.random.uniform(jax.random.fold_in(jax.random.fold_in(rng, 6), dim), (parts,), jnp.float32, low / len(cuts), high / len(cuts))
        level = level * jnp.repeat(jnp.exp(heights), dims[dim] // parts).reshape((-1,) + (1,) * (len(dims) - 1 - dim))
    return level


def length_profile(amount, total, limit, lean):
    weights = [(1 << 20) // math.isqrt(rank ** lean) + 1 for rank in range(2, amount + 1)]
    spare, counts = total - limit - (amount - 1), [1] * (amount - 1)
    while spare > 0:
        free = [i for i in range(amount - 1) if counts[i] < limit]
        whole, remaining = sum([weights[i] for i in free]), spare
        for i in free:
            more = min(limit - counts[i], max(1, remaining * weights[i] // whole), spare)
            counts[i] = counts[i] + more
            spare = spare - more
    return np.array([limit] + counts)


def uneven(rng, count, total, bound, skew):
    if count == 2:
        one = jax.random.randint(rng, (), max(1, total - bound), min(bound, total - 1) + 1)
        return jnp.stack([one, total - one])
    tallies = jnp.asarray(length_profile(count, total, bound, skew), jnp.int32)
    twos = (count - 1) // 2
    giver, taker = tallies[1:1 + 2 * twos:2], tallies[2:2 + 2 * twos:2]
    room = jnp.minimum(giver - 1, bound - taker)
    moved = jax.random.randint(jax.random.fold_in(rng, 1), (twos,), 0, 1 << 20) % (room + 1)
    tallies = tallies.at[1:1 + 2 * twos:2].set(giver - moved).at[2:2 + 2 * twos:2].set(taker + moved)
    return tallies[jax.random.permutation(jax.random.fold_in(rng, 2), count)]


def gaussian(stream_key, dims, scale, limit, shards=(), held_as=jnp.bfloat16):
    entries = scale * jax.random.normal(stream_key, dims, jnp.float32)
    if shards:
        entries = entries * block_scale(stream_key, dims, shards, -0.22, 0.18)
    return jnp.clip(entries, -limit, limit).astype(held_as)


def setup_inputs(seed: int = 0) -> dict:
    keys = jax.random.split(jax.random.key(seed), 13)
    frames = gaussian(keys[0], (FRAMES, DA), 1.0, 6.0, ((0, 4), (1, 4)))
    projector = gaussian(keys[1], (DA, MODEL_WIDTH), DA ** -0.5, 0.078125, ((0, 4), (1, 2)))
    text_token_embedding = gaussian(keys[2], (TOKENS, MODEL_WIDTH), 1.0, 6.0, ((0, 16), (1, 2)))
    norm_gain_vector = jnp.clip(1.0 + 0.18 * jax.random.normal(keys[3], (MODEL_WIDTH,), jnp.float32), 0.1, 1.9)
    frozen = gaussian(keys[4], (MODEL_WIDTH, VALUE_WIDTH), MODEL_WIDTH ** -0.5, 0.0625, ((0, 4), (1, 2)))
    adapter_down_map = gaussian(keys[5], (MODEL_WIDTH, ADAPTER_RANK), MODEL_WIDTH ** -0.5, 0.0625, ((0, 4),))
    adapter_up_map = gaussian(keys[6], (ADAPTER_RANK, VALUE_WIDTH), ADAPTER_RANK ** -0.5, 0.75, ((1, 2),))
    clip_frame_length = draw_clip_frame_length(jax.random.fold_in(keys[12], 71), 0)
    audio_first_token = draw_audio_first_token(jax.random.fold_in(keys[12], 71), 0)
    segment_document_index = jnp.searchsorted(jnp.cumsum(uneven(keys[9], DOCS, TOKENS, 256, 1)), jnp.arange(TOKENS), side="right").astype(jnp.int32)
    keep_document_flags = touch_ends((jax.random.randint(keys[10], (DOCS,), 0, 4) < 3).astype(jnp.int32), jax.random.fold_in(keys[10], 1), 0, 1)
    cotangent = gaussian(keys[11], (TOKENS, VALUE_WIDTH), TOKENS ** -0.5, 0.09375, ((0, 16), (1, 2)))
    return dict(frames=frames, projector=projector, text_token_embedding=text_token_embedding, norm_gain_vector=norm_gain_vector, frozen=frozen, adapter_down_map=adapter_down_map, adapter_up_map=adapter_up_map, clip_frame_length=clip_frame_length, audio_first_token=audio_first_token, segment_document_index=segment_document_index, keep_document_flags=keep_document_flags, cotangent=cotangent)


adapter_scale = 2.0
norm_eps = 1e-05

def reference(frames, projector, text_token_embedding, norm_gain_vector, frozen, adapter_down_map, adapter_up_map, clip_frame_length, audio_first_token, segment_document_index, keep_document_flags, cotangent):
    feat_block = DA // N_GRP
    embed_sum = jnp.zeros((FRAMES, MODEL_WIDTH), jnp.float32)
    for block_id in range(N_GRP):
        low_edge = block_id * feat_block
        partial_sum = jnp.dot(frames[:, low_edge:low_edge + feat_block], projector[low_edge:low_edge + feat_block], preferred_element_type=jnp.float32).astype(jnp.bfloat16)
        partial_sum = lax.optimization_barrier(partial_sum)
        embed_sum = embed_sum + partial_sum.astype(jnp.float32)
    embedded = embed_sum.astype(jnp.bfloat16)
    starts_grid = jnp.cumsum(clip_frame_length, axis=2) - clip_frame_length
    ends_grid = jnp.cumsum(clip_frame_length, axis=2)
    frame_local = lax.broadcasted_iota(jnp.int32, (N_FSDP, N_GRP, FRAMES_DEV), 2)
    clip_index = lax.optimization_barrier(jnp.sum((ends_grid[:, :, None, :] <= frame_local[:, :, :, None]).astype(jnp.int32), axis=3))
    onehot = clip_index[:, :, :, None] == lax.broadcasted_iota(jnp.int32, (1, 1, 1, N_GRP), 3)
    clip_start = lax.optimization_barrier(jnp.sum(jnp.where(onehot, starts_grid[:, :, None, :], 0), axis=3))
    token_start = lax.optimization_barrier(jnp.sum(jnp.where(onehot, audio_first_token[:, :, None, :], 0), axis=3))
    fsdp_iota = lax.broadcasted_iota(jnp.int32, (N_FSDP, N_GRP, FRAMES_DEV), 0)
    token_index = (clip_index * N_FSDP + fsdp_iota) * TOK_DEV + token_start + frame_local - clip_start
    token_flattened = token_index.reshape(FRAMES).astype(jnp.int32)
    inputs = text_token_embedding.at[token_flattened].set(embedded)
    widened = inputs.astype(jnp.float32)
    mean_sq = lax.optimization_barrier(jnp.mean(widened * widened, axis=1))
    inv_rms = lax.rsqrt(mean_sq + norm_eps)
    normalized_input = (widened * inv_rms[:, None] * norm_gain_vector[None, :]).astype(jnp.bfloat16)
    base_output = jnp.dot(normalized_input, frozen, preferred_element_type=jnp.float32)
    lower_rank_rows = jnp.dot(normalized_input, adapter_down_map, preferred_element_type=jnp.float32)
    lower_halfway = lower_rank_rows.astype(jnp.bfloat16)
    value_output = (base_output + adapter_scale * jnp.dot(lower_halfway, adapter_up_map, preferred_element_type=jnp.float32)).astype(jnp.bfloat16)
    weight_tok = keep_document_flags[segment_document_index]
    output_gradient = cotangent * weight_tok.astype(jnp.bfloat16)[:, None]
    up_map_gradient = adapter_scale * jnp.dot(lower_halfway.T, output_gradient, preferred_element_type=jnp.float32)
    adapter_gradient = adapter_scale * jnp.dot(output_gradient, adapter_up_map.T, preferred_element_type=jnp.float32)
    adapter_halfway = adapter_gradient.astype(jnp.bfloat16)
    row_dot_products = lax.optimization_barrier(jnp.sum(output_gradient.astype(jnp.float32) * base_output, axis=1)) + lax.optimization_barrier(jnp.sum(adapter_gradient * lower_rank_rows, axis=1))
    down_map_gradient = jnp.dot(normalized_input.T, adapter_halfway, preferred_element_type=jnp.float32)
    audio_grad = output_gradient[token_flattened]
    tp_cols = VALUE_WIDTH // N_TP
    spread_rows = jnp.zeros((FRAMES, MODEL_WIDTH), jnp.float32)
    for block_id in range(N_TP):
        low_edge = block_id * tp_cols
        partial_sum = jnp.dot(audio_grad[:, low_edge:low_edge + tp_cols], frozen[:, low_edge:low_edge + tp_cols].T, preferred_element_type=jnp.float32).astype(jnp.bfloat16)
        partial_sum = lax.optimization_barrier(partial_sum)
        spread_rows = spread_rows + partial_sum.astype(jnp.float32)
    gradient_norm = spread_rows + jnp.dot(adapter_halfway[token_flattened], adapter_down_map.T, preferred_element_type=jnp.float32)
    audio_inv = inv_rms[token_flattened]
    audio_dot = row_dot_products[token_flattened]
    frame_grad = (audio_inv[:, None] * norm_gain_vector[None, :] * gradient_norm - embedded.astype(jnp.float32) * (audio_inv * audio_inv * audio_dot / MODEL_WIDTH)[:, None]).astype(jnp.bfloat16)
    projector_grad = jnp.dot(frames.T, frame_grad, preferred_element_type=jnp.float32)
    return (value_output, projector_grad, down_map_gradient, up_map_gradient)
```

```python
import jax
import jax.numpy as jnp
from jax import lax
from jax.sharding import PartitionSpec as P

adapter_scale = 2.0
norm_eps = 1e-05
plane = ("fsdp", "tp")


def contract_leading(left_side, right_side):
    return lax.dot_general(
        left_side, right_side, (((0,), (0,)), ((), ())), preferred_element_type=jnp.float32
    )


def contract_trailing(left_side, right_side):
    return lax.dot_general(
        left_side, right_side, (((1,), (1,)), ((), ())), preferred_element_type=jnp.float32
    )


def block_perm(f_size, t_size, shift):
    pairs = []
    for f_src in range(f_size):
        for t_src in range(t_size):
            b = f_src * t_size + (t_src + shift) % t_size
            pairs.append((f_src * t_size + t_src, (b % f_size) * t_size + b // f_size))
    return pairs


def shards(
    frames,
    projector,
    text_token_embedding,
    norm_gain_vector,
    frozen,
    adapter_down_map,
    adapter_up_map,
    clip_frame_length,
    audio_first_token,
    segment_document_index,
    keep_document_flags,
    cotangent,
):
    g_idx, f_idx, t_idx = lax.axis_index("grp"), lax.axis_index("fsdp"), lax.axis_index("tp")
    f_size, t_size = lax.axis_size("fsdp"), lax.axis_size("tp")
    tok, width = text_token_embedding.shape
    groups = clip_frame_length.shape[1]
    block_frames = frames.shape[0]
    per_group = block_frames // groups
    cols = width // f_size
    full_width = width * t_size
    v_shard = frozen.shape[1]
    v_full = v_shard * t_size
    rank = adapter_down_map.shape[1]

    frames_all = lax.all_gather(frames, "fsdp", axis=0, tiled=True)
    clips = lax.all_gather(jnp.stack([clip_frame_length[0], audio_first_token[0]]), "fsdp", axis=0)
    text = lax.all_to_all(
        text_token_embedding.reshape(tok, f_size, cols).transpose(1, 0, 2),
        "fsdp",
        split_axis=0,
        concat_axis=0,
        tiled=True,
    )

    own_block = t_idx * f_size + f_idx
    own_j = lax.rem(own_block, t_size)
    frozen_own = jnp.zeros((cols, v_full), jnp.bfloat16)
    for shift in range(t_size):
        j = lax.rem(t_idx + shift, t_size)
        piece = lax.ppermute(
            lax.dynamic_slice_in_dim(frozen, j * cols, cols, 0),
            plane,
            block_perm(f_size, t_size, shift),
        )
        t_src = lax.rem(own_j - shift + t_size, t_size)
        frozen_own = lax.dynamic_update_slice_in_dim(frozen_own, piece, t_src * v_shard, 1)
    down_own = lax.ppermute(
        lax.dynamic_slice_in_dim(adapter_down_map, t_idx * cols, cols, 0),
        plane,
        block_perm(f_size, t_size, 0),
    )
    gain_own = lax.dynamic_slice_in_dim(norm_gain_vector, t_idx * width + f_idx * cols, cols, 0)

    sizes, firsts = clips[:, 0], clips[:, 1]
    ends = jnp.cumsum(sizes, axis=2)
    pick = lax.broadcasted_iota(jnp.int32, sizes.shape, 2) == g_idx
    size_in = jnp.sum(jnp.where(pick, sizes, 0), axis=2)
    start_in = jnp.sum(jnp.where(pick, ends - sizes, 0), axis=2)
    first_in = jnp.sum(jnp.where(pick, firsts, 0), axis=2)
    base_row = lax.broadcasted_iota(jnp.int32, size_in.shape, 1) * per_group + start_in
    token_iota = lax.broadcasted_iota(jnp.int32, (f_size, tok, groups), 1)
    offset = token_iota - first_in[:, None, :]
    live = (offset >= 0) & (offset < size_in[:, None, :])
    is_audio = jnp.any(live, axis=2)
    row = jnp.sum(jnp.where(live, base_row[:, None, :] + offset, 0), axis=2)
    row = jnp.where(is_audio, row, -1)
    frame_iota = lax.broadcasted_iota(jnp.int32, (f_size, tok, block_frames), 2)
    take = (row[:, :, None] == frame_iota).astype(jnp.bfloat16)
    take_own = lax.dynamic_index_in_dim(take, f_idx, 0, keepdims=False)

    doc_iota = lax.broadcasted_iota(jnp.int32, (tok, keep_document_flags.shape[0]), 1)
    weight_tok = jnp.sum(
        jnp.where(segment_document_index[:, None] == doc_iota, keep_document_flags[None, :], 0),
        axis=1,
    )
    grad_out = cotangent * weight_tok.astype(jnp.bfloat16)[:, None]
    both = lax.all_gather(
        jnp.concatenate([grad_out, adapter_up_map], axis=0), "tp", axis=1, tiled=True
    )
    grad_full, up_full = both[:tok], both[tok:]
    lora_tok = (adapter_scale * contract_trailing(grad_full, up_full)).astype(jnp.bfloat16)
    lora_plane = lax.all_gather(lora_tok, "fsdp", axis=0, tiled=True)
    grad_rows = lax.psum(contract_leading(take_own, grad_full).astype(jnp.bfloat16), "grp")
    grad_rows = lax.all_gather(grad_rows, "fsdp", axis=0, tiled=True)
    lora_rows = (adapter_scale * contract_trailing(grad_rows, up_full)).astype(jnp.bfloat16)
    grad_norm = contract_trailing(grad_rows, frozen_own) + contract_trailing(lora_rows, down_own)

    projector_own = lax.dynamic_slice_in_dim(projector, f_idx * cols, cols, 1)
    embedded = lax.psum(
        jnp.dot(frames_all, projector_own, preferred_element_type=jnp.float32).astype(jnp.bfloat16),
        "grp",
    )
    audio = lax.dot_general(
        take,
        embedded.reshape(f_size, block_frames, cols),
        (((2,), (1,)), ((0,), (0,))),
        preferred_element_type=jnp.float32,
    ).astype(jnp.bfloat16)
    x = jnp.where(is_audio[:, :, None], audio, text).reshape(f_size * tok, cols)
    x32 = x.astype(jnp.float32)
    e32 = embedded.astype(jnp.float32)
    stats = lax.psum(
        jnp.concatenate(
            [
                jnp.sum(x32 * x32, axis=1),
                jnp.sum(e32 * e32, axis=1),
                jnp.sum(e32 * gain_own[None, :] * grad_norm, axis=1),
            ]
        ),
        plane,
    )
    n_tok, n_frames = f_size * tok, f_size * block_frames
    inv_tok = lax.rsqrt(stats[:n_tok] / full_width + norm_eps)
    inv_frame = lax.rsqrt(stats[n_tok : n_tok + n_frames] / full_width + norm_eps)
    dots = inv_frame * stats[n_tok + n_frames :]
    frame_grad = (
        (inv_frame[:, None] * gain_own[None, :]) * grad_norm
        - e32 * (inv_frame * inv_frame * dots / full_width)[:, None]
    ).astype(jnp.bfloat16)
    frame_grad = lax.all_gather(frame_grad, "fsdp", axis=1, tiled=True)
    projector_grad = contract_leading(frames_all, frame_grad)

    normed = (x32 * inv_tok[:, None] * gain_own[None, :]).astype(jnp.bfloat16)
    low_part = jnp.dot(normed, down_own, preferred_element_type=jnp.float32)
    value_part = jnp.dot(normed, frozen_own, preferred_element_type=jnp.float32)
    value_part = value_part + adapter_scale * jnp.dot(
        low_part.astype(jnp.bfloat16), up_full, preferred_element_type=jnp.float32
    )
    value_part = value_part.astype(jnp.bfloat16).reshape(f_size, tok, t_size, v_shard)
    low_send = jnp.broadcast_to(
        low_part.astype(jnp.bfloat16).reshape(f_size, tok, 1, rank), (f_size, tok, t_size, rank)
    )
    sent = (
        jnp.concatenate([value_part, low_send], axis=3)
        .transpose(0, 2, 1, 3)
        .reshape(f_size * t_size, tok, v_shard + rank)
    )
    got = lax.all_to_all(sent, plane, split_axis=0, concat_axis=0, tiled=True)
    total = jnp.sum(got.astype(jnp.float32), axis=0)
    value_output = total[:, :v_shard].astype(jnp.bfloat16)
    low_half = total[:, v_shard:].astype(jnp.bfloat16)

    up_part = adapter_scale * contract_leading(low_half, grad_out)
    down_part = contract_leading(normed, lora_plane)
    down_sum, up_sum = lax.psum((down_part, up_part), "grp")
    gathered = lax.all_gather(
        jnp.concatenate([down_sum, up_sum.reshape(-1, rank)], axis=0), "fsdp", axis=0
    )
    down_map_gradient = gathered[:, :cols].reshape(width, rank)
    up_map_gradient = jnp.sum(gathered[:, cols:], axis=0).reshape(rank, v_shard)
    return (value_output, projector_grad, down_map_gradient, up_map_gradient)


def solution(mesh):
    in_specs = (
        P("fsdp", "grp"),
        P("grp", "tp"),
        P(("grp", "fsdp"), "tp"),
        P(),
        P("fsdp", "tp"),
        P("fsdp", None),
        P(None, "tp"),
        P("fsdp", None, None),
        P("fsdp", None, None),
        P(("grp", "fsdp")),
        P(),
        P(("grp", "fsdp"), "tp"),
    )
    out_specs = (P(("grp", "fsdp"), "tp"), P("grp", "tp"), P("tp", None), P(None, "tp"))
    return jax.shard_map(shards, mesh=mesh, in_specs=in_specs, out_specs=out_specs, check_vma=False)
```

```python
import functools
import math

import jax
import jax.numpy as jnp
from jax import lax
from jax.experimental import pallas as pl
from jax.experimental.pallas import tpu as pltpu
from jax.sharding import PartitionSpec as P

adapter_scale = 2.0
norm_eps = 1e-05
plane = ("fsdp", "tp")

MESH = pl.DeviceIdType.MESH
VMEM = pl.BlockSpec(memory_space=pltpu.VMEM)
DMA = pltpu.SemaphoreType.DMA
VMEM_LIMIT = 48 * 1024 * 1024


def push(src, dst, send_sem, recv_sem, device_id):
    return pltpu.make_async_remote_copy(
        src_ref=src,
        dst_ref=dst,
        send_sem=send_sem,
        recv_sem=recv_sem,
        device_id=device_id,
        device_id_type=MESH,
    )


def greet_plane(f_size, t_size):
    me = lax.axis_index("fsdp") * t_size + lax.axis_index("tp")
    barrier = pltpu.get_barrier_semaphore()
    for k in range(1, f_size * t_size):
        p = lax.rem(me + k, f_size * t_size)
        where = {"fsdp": lax.div(p, t_size), "tp": lax.rem(p, t_size)}
        pl.semaphore_signal(barrier, inc=1, device_id=where, device_id_type=MESH)
    pl.semaphore_wait(barrier, f_size * t_size - 1)


def exchange_kernel(
    f_size,
    t_size,
    frames_ref,
    text_ref,
    frozen_ref,
    frames_out,
    text_out,
    frozen_out,
    send_a,
    recv_a,
    send_b,
    recv_b,
    send_w,
    recv_w,
    local,
):
    f, t = lax.axis_index("fsdp"), lax.axis_index("tp")
    rows = frames_ref.shape[0]
    tok = text_ref.shape[0]
    cols = text_out.shape[1]
    v = frozen_ref.shape[1]
    greet_plane(f_size, t_size)

    def columns(i, size):
        return pl.ds(pl.multiple_of(i * size, 128), size)

    copies = []
    for k in range(1, f_size):
        p = lax.rem(f + k, f_size)
        copies.append(
            push(
                frames_ref,
                frames_out.at[pl.ds(f * rows, rows)],
                send_a.at[k - 1],
                recv_a.at[k - 1],
                {"fsdp": p},
            )
        )
    for k in range(1, f_size):
        p = lax.rem(f + k, f_size)
        copies.append(
            push(
                text_ref.at[:, columns(p, cols)],
                text_out.at[pl.ds(f * tok, tok)],
                send_b.at[k - 1],
                recv_b.at[k - 1],
                {"fsdp": p},
            )
        )
    for c in copies:
        c.start()
    own = [
        pltpu.make_async_copy(frames_ref, frames_out.at[pl.ds(f * rows, rows)], local.at[0]),
        pltpu.make_async_copy(
            text_ref.at[:, columns(f, cols)], text_out.at[pl.ds(f * tok, tok)], local.at[1]
        ),
    ]
    for c in own:
        c.start()
    weights = []
    for j in range(t_size):
        b = f * t_size + j
        d_f, d_t = lax.rem(b, f_size), lax.div(b, f_size)
        mine = jnp.logical_and(d_f == f, d_t == t)
        src = frozen_ref.at[pl.ds(j * cols, cols)]
        dst = frozen_out.at[:, columns(t, v)]
        far = push(src, dst, send_w.at[j], recv_w.at[t], {"fsdp": d_f, "tp": d_t})
        near = pltpu.make_async_copy(src, dst, local.at[2])
        weights.append((mine, far, near))
        pl.when(jnp.logical_not(mine))(far.start)
        pl.when(mine)(near.start)
    for c in own:
        c.wait()
    for c in copies:
        c.wait_recv()
        c.wait_send()
    for mine, far, near in weights:
        pl.when(jnp.logical_not(mine))(far.wait_send)
        pl.when(mine)(near.wait)
    source = lax.div(t * f_size + f, t_size)
    for ts in range(t_size):
        arrive = push(
            frozen_ref.at[pl.ds(0, cols)],
            frozen_out.at[:, pl.ds(ts * v, v)],
            send_w.at[0],
            recv_w.at[ts],
            {"fsdp": lax.rem(f + 1, f_size)},
        )
        pl.when(jnp.logical_not(jnp.logical_and(source == f, t == ts)))(arrive.wait_recv)


def exchange(frames, text, frozen, f_size, t_size):
    cols = text.shape[1] // f_size
    return pl.pallas_call(
        functools.partial(exchange_kernel, f_size, t_size),
        out_shape=(
            jax.ShapeDtypeStruct((frames.shape[0] * f_size, frames.shape[1]), frames.dtype),
            jax.ShapeDtypeStruct((text.shape[0] * f_size, cols), text.dtype),
            jax.ShapeDtypeStruct((cols, frozen.shape[1] * t_size), frozen.dtype),
        ),
        in_specs=[VMEM] * 3,
        out_specs=(VMEM,) * 3,
        scratch_shapes=[DMA((f_size - 1,))] * 4 + [DMA((t_size,))] * 2 + [DMA((3,))],
        compiler_params=pltpu.CompilerParams(
            collective_id=0, has_side_effects=True, vmem_limit_bytes=VMEM_LIMIT
        ),
        name="exchange",
    )(frames, text, frozen)


def line_kernel(n, chunks, x_ref, o_ref, from_left, from_right, to_right, to_left, *sems):
    send_r, recv_r, send_l, recv_l = sems
    g = lax.axis_index("grp")
    rows = x_ref.shape[0] // chunks
    right, left = jnp.minimum(g + 1, n - 1), jnp.maximum(g - 1, 0)
    has_left, has_right = g > 0, g < n - 1
    barrier = pltpu.get_barrier_semaphore()

    @pl.when(has_left)
    def _():
        pl.semaphore_signal(barrier, inc=1, device_id={"grp": left}, device_id_type=MESH)

    @pl.when(has_right)
    def _():
        pl.semaphore_signal(barrier, inc=1, device_id={"grp": right}, device_id_type=MESH)

    pl.semaphore_wait(barrier, has_left.astype(jnp.int32) + has_right.astype(jnp.int32))

    def part(c):
        return pl.ds(pl.multiple_of(c * rows, rows), rows)

    def rightward(c):
        return push(
            to_right.at[part(c)], from_left.at[part(c)], send_r.at[c], recv_r.at[c], {"grp": right}
        )

    def leftward(c):
        return push(
            to_left.at[part(c)], from_right.at[part(c)], send_l.at[c], recv_l.at[c], {"grp": left}
        )

    def step(c, has_in, has_out, copy, came, going):
        fits = jnp.logical_and(c >= 0, c < chunks)

        @pl.when(jnp.logical_and(fits, has_in))
        def _():
            copy(c).wait_recv()

        @pl.when(jnp.logical_and(fits, jnp.logical_and(has_in, has_out)))
        def _():
            total = came[part(c)].astype(jnp.float32) + x_ref[part(c)].astype(jnp.float32)
            going[part(c)] = total.astype(going.dtype)
            copy(c).start()

        @pl.when(jnp.logical_and(fits, jnp.logical_and(jnp.logical_not(has_in), has_out)))
        def _():
            going[part(c)] = x_ref[part(c)]
            copy(c).start()

    def body(i, carry):
        step(i - g, has_left, has_right, rightward, from_left, to_right)
        step(i - (n - 1 - g), has_right, has_left, leftward, from_right, to_left)
        return carry

    lax.fori_loop(0, chunks + n - 1, body, 0)

    def finish(c, carry):
        @pl.when(jnp.logical_not(has_left))
        def _():
            total = x_ref[part(c)].astype(jnp.float32) + from_right[part(c)].astype(jnp.float32)
            o_ref[part(c)] = total.astype(o_ref.dtype)

        @pl.when(jnp.logical_not(has_right))
        def _():
            total = x_ref[part(c)].astype(jnp.float32) + from_left[part(c)].astype(jnp.float32)
            o_ref[part(c)] = total.astype(o_ref.dtype)

        @pl.when(jnp.logical_and(has_left, has_right))
        def _():
            total = from_left[part(c)].astype(jnp.float32) + from_right[part(c)].astype(jnp.float32)
            total = total + x_ref[part(c)].astype(jnp.float32)
            o_ref[part(c)] = total.astype(o_ref.dtype)

        @pl.when(has_right)
        def _():
            rightward(c).wait_send()

        @pl.when(has_left)
        def _():
            leftward(c).wait_send()

        return carry

    lax.fori_loop(0, chunks, finish, 0)


def line_sum(x, n, chunks, collective_id):
    return pl.pallas_call(
        functools.partial(line_kernel, n, chunks),
        out_shape=jax.ShapeDtypeStruct(x.shape, x.dtype),
        in_specs=[VMEM],
        out_specs=VMEM,
        scratch_shapes=[pltpu.VMEM(x.shape, x.dtype)] * 4 + [DMA((chunks,))] * 4,
        compiler_params=pltpu.CompilerParams(
            collective_id=collective_id, has_side_effects=True, vmem_limit_bytes=VMEM_LIMIT
        ),
        name="line_sum",
    )(x)


def plane_sum_kernel(f_size, t_size, x_ref, o_ref, slots, send, recv):
    count = f_size * t_size
    me = lax.axis_index("fsdp") * t_size + lax.axis_index("tp")
    greet_plane(f_size, t_size)
    copies = []
    for k in range(1, count):
        p = lax.rem(me + k, count)
        where = {"fsdp": lax.div(p, t_size), "tp": lax.rem(p, t_size)}
        copies.append(push(x_ref, slots.at[k - 1], send.at[k - 1], recv.at[k - 1], where))
        copies[-1].start()
    total = x_ref[...]
    for k in range(1, count):
        copies[k - 1].wait_recv()
        total = total + slots[k - 1]
    o_ref[...] = total
    for c in copies:
        c.wait_send()


def plane_sum(x, f_size, t_size):
    count = f_size * t_size - 1
    return pl.pallas_call(
        functools.partial(plane_sum_kernel, f_size, t_size),
        out_shape=jax.ShapeDtypeStruct(x.shape, x.dtype),
        in_specs=[VMEM],
        out_specs=VMEM,
        scratch_shapes=[pltpu.VMEM((count,) + x.shape, x.dtype), DMA((count,)), DMA((count,))],
        compiler_params=pltpu.CompilerParams(collective_id=2, has_side_effects=True),
        name="plane_sum",
    )(x)


def gather_kernel(f_size, x_ref, o_ref, send, recv):
    f = lax.axis_index("fsdp")
    barrier = pltpu.get_barrier_semaphore()
    for k in range(1, f_size):
        where = {"fsdp": lax.rem(f + k, f_size)}
        pl.semaphore_signal(barrier, inc=1, device_id=where, device_id_type=MESH)
    pl.semaphore_wait(barrier, f_size - 1)
    copies = []
    for k in range(1, f_size):
        where = {"fsdp": lax.rem(f + k, f_size)}
        copies.append(push(x_ref, o_ref.at[f], send.at[k - 1], recv.at[k - 1], where))
        copies[-1].start()
    o_ref[f] = x_ref[...]
    for c in copies:
        c.wait_recv()
        c.wait_send()


def fsdp_gather(x, f_size, collective_id):
    return pl.pallas_call(
        functools.partial(gather_kernel, f_size),
        out_shape=jax.ShapeDtypeStruct((f_size,) + x.shape, x.dtype),
        in_specs=[VMEM],
        out_specs=VMEM,
        scratch_shapes=[DMA((f_size - 1,)), DMA((f_size - 1,))],
        compiler_params=pltpu.CompilerParams(collective_id=collective_id, has_side_effects=True),
        name="fsdp_gather",
    )(x)


def product_kernel(a_ref, b_ref, o_ref):
    o_ref[...] = jnp.dot(a_ref[...], b_ref[...], preferred_element_type=jnp.float32)


def product(a, b):
    m, k = a.shape
    n = b.shape[1]
    bm, bn = math.gcd(m, 256), math.gcd(n, 1024)
    return pl.pallas_call(
        product_kernel,
        out_shape=jax.ShapeDtypeStruct((m, n), jnp.float32),
        grid=(n // bn, m // bm),
        in_specs=[
            pl.BlockSpec((bm, k), lambda j, i: (i, 0)),
            pl.BlockSpec((k, bn), lambda j, i: (0, j)),
        ],
        out_specs=pl.BlockSpec((bm, bn), lambda j, i: (i, j)),
        compiler_params=pltpu.CompilerParams(vmem_limit_bytes=VMEM_LIMIT),
        name="product",
    )(a, b)


def contract_leading(left_side, right_side):
    return lax.dot_general(
        left_side, right_side, (((0,), (0,)), ((), ())), preferred_element_type=jnp.float32
    )


def contract_trailing(left_side, right_side):
    return lax.dot_general(
        left_side, right_side, (((1,), (1,)), ((), ())), preferred_element_type=jnp.float32
    )


def block_perm(f_size, t_size, shift):
    pairs = []
    for f_src in range(f_size):
        for t_src in range(t_size):
            b = f_src * t_size + (t_src + shift) % t_size
            pairs.append((f_src * t_size + t_src, (b % f_size) * t_size + b // f_size))
    return pairs


def shards(
    frames,
    projector,
    text_token_embedding,
    norm_gain_vector,
    frozen,
    adapter_down_map,
    adapter_up_map,
    clip_frame_length,
    audio_first_token,
    segment_document_index,
    keep_document_flags,
    cotangent,
):
    g_idx, f_idx, t_idx = lax.axis_index("grp"), lax.axis_index("fsdp"), lax.axis_index("tp")
    f_size, t_size = lax.axis_size("fsdp"), lax.axis_size("tp")
    tok, width = text_token_embedding.shape
    groups = clip_frame_length.shape[1]
    block_frames = frames.shape[0]
    per_group = block_frames // groups
    cols = width // f_size
    full_width = width * t_size
    v_shard = frozen.shape[1]
    v_full = v_shard * t_size
    rank = adapter_down_map.shape[1]

    clips = lax.all_gather(jnp.stack([clip_frame_length[0], audio_first_token[0]]), "fsdp", axis=0)
    down_own = lax.ppermute(
        lax.dynamic_slice_in_dim(adapter_down_map, t_idx * cols, cols, 0),
        plane,
        block_perm(f_size, t_size, 0),
    )
    gain_own = lax.dynamic_slice_in_dim(norm_gain_vector, t_idx * width + f_idx * cols, cols, 0)

    sizes, firsts = clips[:, 0], clips[:, 1]
    ends = jnp.cumsum(sizes, axis=2)
    pick = lax.broadcasted_iota(jnp.int32, sizes.shape, 2) == g_idx
    size_in = jnp.sum(jnp.where(pick, sizes, 0), axis=2)
    start_in = jnp.sum(jnp.where(pick, ends - sizes, 0), axis=2)
    first_in = jnp.sum(jnp.where(pick, firsts, 0), axis=2)
    base_row = lax.broadcasted_iota(jnp.int32, size_in.shape, 1) * per_group + start_in
    token_iota = lax.broadcasted_iota(jnp.int32, (f_size, tok, groups), 1)
    offset = token_iota - first_in[:, None, :]
    live = (offset >= 0) & (offset < size_in[:, None, :])
    is_audio = jnp.any(live, axis=2)
    row = jnp.sum(jnp.where(live, base_row[:, None, :] + offset, 0), axis=2)
    row = jnp.where(is_audio, row, -1)
    frame_iota = lax.broadcasted_iota(jnp.int32, (f_size, tok, block_frames), 2)
    take = (row[:, :, None] == frame_iota).astype(jnp.bfloat16)
    take_own = lax.dynamic_index_in_dim(take, f_idx, 0, keepdims=False)

    doc_iota = lax.broadcasted_iota(jnp.int32, (tok, keep_document_flags.shape[0]), 1)
    weight_tok = jnp.sum(
        jnp.where(segment_document_index[:, None] == doc_iota, keep_document_flags[None, :], 0),
        axis=1,
    )
    grad_out = cotangent * weight_tok.astype(jnp.bfloat16)[:, None]
    both = lax.all_gather(
        jnp.concatenate([grad_out, adapter_up_map], axis=0), "tp", axis=1, tiled=True
    )
    grad_full, up_full = both[:tok], both[tok:]
    lora_tok = (adapter_scale * contract_trailing(grad_full, up_full)).astype(jnp.bfloat16)
    lora_plane = lax.all_gather(lora_tok, "fsdp", axis=0, tiled=True)
    grad_rows = lax.psum(contract_leading(take_own, grad_full).astype(jnp.bfloat16), "grp")

    frames_all, text, frozen_own = exchange(frames, text_token_embedding, frozen, f_size, t_size)
    text = text.reshape(f_size, tok, cols)
    grad_rows, frames_all = lax.optimization_barrier((grad_rows, frames_all))
    grad_rows = lax.all_gather(grad_rows, "fsdp", axis=0, tiled=True)
    lora_rows = (adapter_scale * contract_trailing(grad_rows, up_full)).astype(jnp.bfloat16)
    grad_norm = contract_trailing(grad_rows, frozen_own) + contract_trailing(lora_rows, down_own)

    projector_own = lax.dynamic_slice_in_dim(projector, f_idx * cols, cols, 1)
    embedded = line_sum(
        jnp.dot(frames_all, projector_own, preferred_element_type=jnp.float32).astype(jnp.bfloat16),
        lax.axis_size("grp"),
        16,
        1,
    )
    audio = lax.dot_general(
        take,
        embedded.reshape(f_size, block_frames, cols),
        (((2,), (1,)), ((0,), (0,))),
        preferred_element_type=jnp.float32,
    ).astype(jnp.bfloat16)
    x = jnp.where(is_audio[:, :, None], audio, text).reshape(f_size * tok, cols)
    x32 = x.astype(jnp.float32)
    e32 = embedded.astype(jnp.float32)
    stats = jnp.concatenate(
        [
            jnp.sum(x32 * x32, axis=1),
            jnp.sum(e32 * e32, axis=1),
            jnp.sum(e32 * gain_own[None, :] * grad_norm, axis=1),
        ]
    )
    stats = jnp.pad(stats, (0, -stats.shape[0] % 1024)).reshape(-1, 128)
    stats = plane_sum(stats, f_size, t_size).reshape(-1)
    n_tok, n_frames = f_size * tok, f_size * block_frames
    inv_tok = lax.rsqrt(stats[:n_tok] / full_width + norm_eps)
    inv_frame = lax.rsqrt(stats[n_tok : n_tok + n_frames] / full_width + norm_eps)
    dots = inv_frame * stats[n_tok + n_frames : n_tok + 2 * n_frames]
    frame_grad = (
        (inv_frame[:, None] * gain_own[None, :]) * grad_norm
        - e32 * (inv_frame * inv_frame * dots / full_width)[:, None]
    ).astype(jnp.bfloat16)
    frame_grad = lax.all_gather(frame_grad, "fsdp", axis=1, tiled=True)
    projector_grad = product(frames_all.T, frame_grad)

    normed = (x32 * inv_tok[:, None] * gain_own[None, :]).astype(jnp.bfloat16)
    low_part = jnp.dot(normed, down_own, preferred_element_type=jnp.float32)
    value_part = jnp.dot(normed, frozen_own, preferred_element_type=jnp.float32)
    value_part = value_part + adapter_scale * jnp.dot(
        low_part.astype(jnp.bfloat16), up_full, preferred_element_type=jnp.float32
    )
    value_part = value_part.astype(jnp.bfloat16).reshape(f_size, tok, t_size, v_shard)
    low_send = jnp.broadcast_to(
        low_part.astype(jnp.bfloat16).reshape(f_size, tok, 1, rank), (f_size, tok, t_size, rank)
    )
    sent = (
        jnp.concatenate([value_part, low_send], axis=3)
        .transpose(0, 2, 1, 3)
        .reshape(f_size * t_size, tok, v_shard + rank)
    )
    got = lax.all_to_all(sent, plane, split_axis=0, concat_axis=0, tiled=True)
    total = jnp.sum(got.astype(jnp.float32), axis=0)
    value_output = total[:, :v_shard].astype(jnp.bfloat16)
    low_half = total[:, v_shard:].astype(jnp.bfloat16)

    up_part = adapter_scale * contract_leading(low_half, grad_out)
    down_part = contract_leading(normed, lora_plane)
    both_parts = jnp.concatenate([down_part.reshape(-1, 128), up_part.reshape(-1, 128)], axis=0)
    summed = line_sum(both_parts, lax.axis_size("grp"), 4, 3)
    gathered = fsdp_gather(summed, f_size, 4)
    split = cols * rank // 128
    down_map_gradient = gathered[:, :split].reshape(width, rank)
    up_map_gradient = jnp.sum(gathered[:, split:], axis=0).reshape(rank, v_shard)
    return (value_output, projector_grad, down_map_gradient, up_map_gradient)


def solution(mesh):
    in_specs = (
        P("fsdp", "grp"),
        P("grp", "tp"),
        P(("grp", "fsdp"), "tp"),
        P(),
        P("fsdp", "tp"),
        P("fsdp", None),
        P(None, "tp"),
        P("fsdp", None, None),
        P("fsdp", None, None),
        P(("grp", "fsdp")),
        P(),
        P(("grp", "fsdp"), "tp"),
    )
    out_specs = (P(("grp", "fsdp"), "tp"), P("grp", "tp"), P("tp", None), P(None, "tp"))
    return jax.shard_map(shards, mesh=mesh, in_specs=in_specs, out_specs=out_specs, check_vma=False)
```

```python
import functools
import math

import jax
import jax.numpy as jnp
from jax import lax
from jax.experimental import pallas as pl
from jax.experimental.pallas import tpu as pltpu
from jax.sharding import PartitionSpec as P

adapter_scale = 2.0
norm_eps = 1e-05
plane = ("fsdp", "tp")

MESH = pl.DeviceIdType.MESH
VMEM = pl.BlockSpec(memory_space=pltpu.VMEM)
DMA = pltpu.SemaphoreType.DMA
VMEM_LIMIT = 48 * 1024 * 1024


def push(src, dst, send_sem, recv_sem, device_id):
    return pltpu.make_async_remote_copy(
        src_ref=src,
        dst_ref=dst,
        send_sem=send_sem,
        recv_sem=recv_sem,
        device_id=device_id,
        device_id_type=MESH,
    )


def greet_plane(f_size, t_size, barrier):
    me = lax.axis_index("fsdp") * t_size + lax.axis_index("tp")
    for k in range(1, f_size * t_size):
        p = lax.rem(me + k, f_size * t_size)
        where = {"fsdp": lax.div(p, t_size), "tp": lax.rem(p, t_size)}
        pl.semaphore_signal(barrier, inc=1, device_id=where, device_id_type=MESH)


def start_exchange(f_size, t_size, text_ref, frozen_ref, text_out, frozen_out, sems):
    send_b, recv_b, send_w, recv_w, local = sems
    f, t = lax.axis_index("fsdp"), lax.axis_index("tp")
    tok = text_ref.shape[0]
    cols = text_out.shape[1]
    v = frozen_ref.shape[1]

    def columns(i, size):
        return pl.ds(pl.multiple_of(i * size, 128), size)

    weights = []
    for j in range(t_size):
        b = f * t_size + j
        d_f, d_t = lax.rem(b, f_size), lax.div(b, f_size)
        mine = jnp.logical_and(d_f == f, d_t == t)
        src = frozen_ref.at[pl.ds(j * cols, cols)]
        dst = frozen_out.at[:, columns(t, v)]
        far = push(src, dst, send_w.at[j], recv_w.at[t], {"fsdp": d_f, "tp": d_t})
        near = pltpu.make_async_copy(src, dst, local.at[1])
        weights.append((mine, far, near))
        pl.when(jnp.logical_not(mine))(far.start)
        pl.when(mine)(near.start)
    copies = []
    for k in range(1, f_size):
        p = lax.rem(f + k, f_size)
        copies.append(
            push(
                text_ref.at[:, columns(p, cols)],
                text_out.at[pl.ds(f * tok, tok)],
                send_b.at[k - 1],
                recv_b.at[k - 1],
                {"fsdp": p},
            )
        )
        copies[-1].start()
    own = pltpu.make_async_copy(
        text_ref.at[:, columns(f, cols)], text_out.at[pl.ds(f * tok, tok)], local.at[0]
    )
    own.start()

    def finish():
        own.wait()
        for c in copies:
            c.wait_recv()
            c.wait_send()
        for mine, far, near in weights:
            pl.when(jnp.logical_not(mine))(far.wait_send)
            pl.when(mine)(near.wait)
        source = lax.div(t * f_size + f, t_size)
        for ts in range(t_size):
            arrive = push(
                frozen_ref.at[pl.ds(0, cols)],
                frozen_out.at[:, pl.ds(ts * v, v)],
                send_w.at[0],
                recv_w.at[ts],
                {"fsdp": lax.rem(f + 1, f_size)},
            )
            pl.when(jnp.logical_not(jnp.logical_and(source == f, t == ts)))(arrive.wait_recv)

    return finish


def sum_and_exchange_kernel(
    n, chunks, f_size, t_size, x_ref, text_ref, frozen_ref, o_ref, text_out, frozen_out, *scratch
):
    def start():
        return start_exchange(
            f_size, t_size, text_ref, frozen_ref, text_out, frozen_out, scratch[8:]
        )

    line_kernel(n, chunks, x_ref, o_ref, *scratch[:8], plane_sizes=(f_size, t_size), extra=start)


def sum_and_exchange(x, text, frozen, n, f_size, t_size, chunks):
    cols = text.shape[1] // f_size
    return pl.pallas_call(
        functools.partial(sum_and_exchange_kernel, n, chunks, f_size, t_size),
        out_shape=(
            jax.ShapeDtypeStruct(x.shape, x.dtype),
            jax.ShapeDtypeStruct((text.shape[0] * f_size, cols), text.dtype),
            jax.ShapeDtypeStruct((cols, frozen.shape[1] * t_size), frozen.dtype),
        ),
        in_specs=[VMEM] * 3,
        out_specs=(VMEM,) * 3,
        scratch_shapes=[pltpu.VMEM(x.shape, x.dtype)] * 4
        + [DMA((chunks,))] * 4
        + [DMA((f_size - 1,))] * 2
        + [DMA((t_size,))] * 2
        + [DMA((2,))],
        compiler_params=pltpu.CompilerParams(
            collective_id=1, has_side_effects=True, vmem_limit_bytes=VMEM_LIMIT
        ),
        name="sum_and_exchange",
    )(x, text, frozen)


LAG = 2


def line_kernel(n, chunks, x_ref, o_ref, from_left, from_right, to_right, to_left, *sems, **more):
    send_r, recv_r, send_l, recv_l = sems
    plane_sizes, extra = more.get("plane_sizes"), more.get("extra")
    g = lax.axis_index("grp")
    rows = x_ref.shape[0] // chunks
    right, left = jnp.minimum(g + 1, n - 1), jnp.maximum(g - 1, 0)
    has_left, has_right = g > 0, g < n - 1
    barrier = pltpu.get_barrier_semaphore()

    @pl.when(has_left)
    def _():
        pl.semaphore_signal(barrier, inc=1, device_id={"grp": left}, device_id_type=MESH)

    @pl.when(has_right)
    def _():
        pl.semaphore_signal(barrier, inc=1, device_id={"grp": right}, device_id_type=MESH)

    expected = has_left.astype(jnp.int32) + has_right.astype(jnp.int32)
    if extra is not None:
        greet_plane(*plane_sizes, barrier)
        expected = expected + plane_sizes[0] * plane_sizes[1] - 1
    pl.semaphore_wait(barrier, expected)
    end_extra = extra() if extra is not None else None

    def part(c):
        return pl.ds(pl.multiple_of(c * rows, rows), rows)

    def rightward(c):
        return push(
            to_right.at[part(c)], from_left.at[part(c)], send_r.at[c], recv_r.at[c], {"grp": right}
        )

    def leftward(c):
        return push(
            to_left.at[part(c)], from_right.at[part(c)], send_l.at[c], recv_l.at[c], {"grp": left}
        )

    def step(c, has_in, has_out, copy, came, going):
        fits = jnp.logical_and(c >= 0, c < chunks)

        @pl.when(jnp.logical_and(fits, has_in))
        def _():
            copy(c).wait_recv()

        @pl.when(jnp.logical_and(fits, jnp.logical_and(has_in, has_out)))
        def _():
            total = came[part(c)].astype(jnp.float32) + x_ref[part(c)].astype(jnp.float32)
            going[part(c)] = total.astype(going.dtype)
            copy(c).start()

        @pl.when(jnp.logical_and(fits, jnp.logical_and(jnp.logical_not(has_in), has_out)))
        def _():
            going[part(c)] = x_ref[part(c)]
            copy(c).start()

    def body(i, carry):
        step(i - LAG * g, has_left, has_right, rightward, from_left, to_right)
        step(i - LAG * (n - 1 - g), has_right, has_left, leftward, from_right, to_left)
        return carry

    lax.fori_loop(0, chunks + LAG * (n - 1), body, 0)

    def finish(c, carry):
        @pl.when(jnp.logical_not(has_left))
        def _():
            total = x_ref[part(c)].astype(jnp.float32) + from_right[part(c)].astype(jnp.float32)
            o_ref[part(c)] = total.astype(o_ref.dtype)

        @pl.when(jnp.logical_not(has_right))
        def _():
            total = x_ref[part(c)].astype(jnp.float32) + from_left[part(c)].astype(jnp.float32)
            o_ref[part(c)] = total.astype(o_ref.dtype)

        @pl.when(jnp.logical_and(has_left, has_right))
        def _():
            total = from_left[part(c)].astype(jnp.float32) + from_right[part(c)].astype(jnp.float32)
            total = total + x_ref[part(c)].astype(jnp.float32)
            o_ref[part(c)] = total.astype(o_ref.dtype)

        @pl.when(has_right)
        def _():
            rightward(c).wait_send()

        @pl.when(has_left)
        def _():
            leftward(c).wait_send()

        return carry

    lax.fori_loop(0, chunks, finish, 0)
    if end_extra is not None:
        end_extra()


def line_sum(x, n, chunks, collective_id):
    return pl.pallas_call(
        functools.partial(line_kernel, n, chunks),
        out_shape=jax.ShapeDtypeStruct(x.shape, x.dtype),
        in_specs=[VMEM],
        out_specs=VMEM,
        scratch_shapes=[pltpu.VMEM(x.shape, x.dtype)] * 4 + [DMA((chunks,))] * 4,
        compiler_params=pltpu.CompilerParams(
            collective_id=collective_id, has_side_effects=True, vmem_limit_bytes=VMEM_LIMIT
        ),
        name="line_sum",
    )(x)


def plane_sum_kernel(f_size, t_size, x_ref, o_ref, slots, send, recv):
    count = f_size * t_size
    me = lax.axis_index("fsdp") * t_size + lax.axis_index("tp")
    barrier = pltpu.get_barrier_semaphore()
    greet_plane(f_size, t_size, barrier)
    pl.semaphore_wait(barrier, count - 1)
    copies = []
    for k in range(1, count):
        p = lax.rem(me + k, count)
        where = {"fsdp": lax.div(p, t_size), "tp": lax.rem(p, t_size)}
        copies.append(push(x_ref, slots.at[k - 1], send.at[k - 1], recv.at[k - 1], where))
        copies[-1].start()
    total = x_ref[...]
    for k in range(1, count):
        copies[k - 1].wait_recv()
        total = total + slots[k - 1]
    o_ref[...] = total
    for c in copies:
        c.wait_send()


def plane_sum(x, f_size, t_size):
    count = f_size * t_size - 1
    return pl.pallas_call(
        functools.partial(plane_sum_kernel, f_size, t_size),
        out_shape=jax.ShapeDtypeStruct(x.shape, x.dtype),
        in_specs=[VMEM],
        out_specs=VMEM,
        scratch_shapes=[pltpu.VMEM((count,) + x.shape, x.dtype), DMA((count,)), DMA((count,))],
        compiler_params=pltpu.CompilerParams(collective_id=2, has_side_effects=True),
        name="plane_sum",
    )(x)


def gather_kernel(f_size, count, *refs):
    ins, outs, sems = refs[:count], refs[count : 2 * count], refs[2 * count :]
    f = lax.axis_index("fsdp")
    barrier = pltpu.get_barrier_semaphore()
    for k in range(1, f_size):
        where = {"fsdp": lax.rem(f + k, f_size)}
        pl.semaphore_signal(barrier, inc=1, device_id=where, device_id_type=MESH)
    pl.semaphore_wait(barrier, f_size - 1)
    copies = []
    for i in range(count):
        send, recv = sems[2 * i], sems[2 * i + 1]
        for k in range(1, f_size):
            where = {"fsdp": lax.rem(f + k, f_size)}
            copies.append(push(ins[i], outs[i].at[f], send.at[k - 1], recv.at[k - 1], where))
            copies[-1].start()
    for i in range(count):
        outs[i][f] = ins[i][...]
    for c in copies:
        c.wait_recv()
        c.wait_send()


def fsdp_gather(arrays, f_size, collective_id):
    count = len(arrays)
    return pl.pallas_call(
        functools.partial(gather_kernel, f_size, count),
        out_shape=tuple(jax.ShapeDtypeStruct((f_size,) + x.shape, x.dtype) for x in arrays),
        in_specs=[VMEM] * count,
        out_specs=(VMEM,) * count,
        scratch_shapes=[DMA((f_size - 1,))] * (2 * count),
        compiler_params=pltpu.CompilerParams(
            collective_id=collective_id, has_side_effects=True, vmem_limit_bytes=VMEM_LIMIT
        ),
        name="fsdp_gather",
    )(*arrays)


def product_kernel(a_ref, b_ref, o_ref):
    o_ref[...] = jnp.dot(a_ref[...], b_ref[...], preferred_element_type=jnp.float32)


def product(a, b):
    m, k = a.shape
    n = b.shape[1]
    bm, bn = math.gcd(m, 256), math.gcd(n, 1024)
    return pl.pallas_call(
        product_kernel,
        out_shape=jax.ShapeDtypeStruct((m, n), jnp.float32),
        grid=(n // bn, m // bm),
        in_specs=[
            pl.BlockSpec((bm, k), lambda j, i: (i, 0)),
            pl.BlockSpec((k, bn), lambda j, i: (0, j)),
        ],
        out_specs=pl.BlockSpec((bm, bn), lambda j, i: (i, j)),
        compiler_params=pltpu.CompilerParams(vmem_limit_bytes=VMEM_LIMIT),
        name="product",
    )(a, b)


def contract_leading(left_side, right_side):
    return lax.dot_general(
        left_side, right_side, (((0,), (0,)), ((), ())), preferred_element_type=jnp.float32
    )


def contract_trailing(left_side, right_side):
    return lax.dot_general(
        left_side, right_side, (((1,), (1,)), ((), ())), preferred_element_type=jnp.float32
    )


def block_perm(f_size, t_size, shift):
    pairs = []
    for f_src in range(f_size):
        for t_src in range(t_size):
            b = f_src * t_size + (t_src + shift) % t_size
            pairs.append((f_src * t_size + t_src, (b % f_size) * t_size + b // f_size))
    return pairs


def shards(
    frames,
    projector,
    text_token_embedding,
    norm_gain_vector,
    frozen,
    adapter_down_map,
    adapter_up_map,
    clip_frame_length,
    audio_first_token,
    segment_document_index,
    keep_document_flags,
    cotangent,
):
    g_idx, f_idx, t_idx = lax.axis_index("grp"), lax.axis_index("fsdp"), lax.axis_index("tp")
    f_size, t_size = lax.axis_size("fsdp"), lax.axis_size("tp")
    tok, width = text_token_embedding.shape
    groups = clip_frame_length.shape[1]
    block_frames = frames.shape[0]
    per_group = block_frames // groups
    cols = width // f_size
    full_width = width * t_size
    v_shard = frozen.shape[1]
    v_full = v_shard * t_size
    rank = adapter_down_map.shape[1]

    clips = lax.all_gather(jnp.stack([clip_frame_length[0], audio_first_token[0]]), "fsdp", axis=0)
    down_own = lax.ppermute(
        lax.dynamic_slice_in_dim(adapter_down_map, t_idx * cols, cols, 0),
        plane,
        block_perm(f_size, t_size, 0),
    )
    gain_own = lax.dynamic_slice_in_dim(norm_gain_vector, t_idx * width + f_idx * cols, cols, 0)

    sizes, firsts = clips[:, 0], clips[:, 1]
    ends = jnp.cumsum(sizes, axis=2)
    pick = lax.broadcasted_iota(jnp.int32, sizes.shape, 2) == g_idx
    size_in = jnp.sum(jnp.where(pick, sizes, 0), axis=2)
    start_in = jnp.sum(jnp.where(pick, ends - sizes, 0), axis=2)
    first_in = jnp.sum(jnp.where(pick, firsts, 0), axis=2)
    base_row = lax.broadcasted_iota(jnp.int32, size_in.shape, 1) * per_group + start_in
    token_iota = lax.broadcasted_iota(jnp.int32, (f_size, tok, groups), 1)
    offset = token_iota - first_in[:, None, :]
    live = (offset >= 0) & (offset < size_in[:, None, :])
    is_audio = jnp.any(live, axis=2)
    row = jnp.sum(jnp.where(live, base_row[:, None, :] + offset, 0), axis=2)
    row = jnp.where(is_audio, row, -1)
    frame_iota = lax.broadcasted_iota(jnp.int32, (f_size, tok, block_frames), 2)
    take = (row[:, :, None] == frame_iota).astype(jnp.bfloat16)
    take_own = lax.dynamic_index_in_dim(take, f_idx, 0, keepdims=False)

    doc_iota = lax.broadcasted_iota(jnp.int32, (tok, keep_document_flags.shape[0]), 1)
    weight_tok = jnp.sum(
        jnp.where(segment_document_index[:, None] == doc_iota, keep_document_flags[None, :], 0),
        axis=1,
    )
    grad_out = cotangent * weight_tok.astype(jnp.bfloat16)[:, None]
    both = lax.all_gather(
        jnp.concatenate([grad_out, adapter_up_map], axis=0), "tp", axis=1, tiled=True
    )
    grad_full, up_full = both[:tok], both[tok:]
    lora_tok = (adapter_scale * contract_trailing(grad_full, up_full)).astype(jnp.bfloat16)
    grad_rows = lax.psum(contract_leading(take_own, grad_full).astype(jnp.bfloat16), "grp")

    frames_all, lora_plane = fsdp_gather((frames, lora_tok), f_size, 0)
    frames_all = frames_all.reshape(f_size * block_frames, frames.shape[1])
    lora_plane = lora_plane.reshape(f_size * tok, rank)
    grad_rows, frames_all = lax.optimization_barrier((grad_rows, frames_all))
    grad_rows = lax.all_gather(grad_rows, "fsdp", axis=0, tiled=True)

    projector_own = lax.dynamic_slice_in_dim(projector, f_idx * cols, cols, 1)
    embedded, text, frozen_own = sum_and_exchange(
        jnp.dot(frames_all, projector_own, preferred_element_type=jnp.float32).astype(jnp.bfloat16),
        text_token_embedding,
        frozen,
        lax.axis_size("grp"),
        f_size,
        t_size,
        16,
    )
    text = text.reshape(f_size, tok, cols)
    lora_rows = (adapter_scale * contract_trailing(grad_rows, up_full)).astype(jnp.bfloat16)
    grad_norm = contract_trailing(grad_rows, frozen_own) + contract_trailing(lora_rows, down_own)
    audio = lax.dot_general(
        take,
        embedded.reshape(f_size, block_frames, cols),
        (((2,), (1,)), ((0,), (0,))),
        preferred_element_type=jnp.float32,
    ).astype(jnp.bfloat16)
    x = jnp.where(is_audio[:, :, None], audio, text).reshape(f_size * tok, cols)
    x32 = x.astype(jnp.float32)
    e32 = embedded.astype(jnp.float32)
    stats = jnp.concatenate(
        [
            jnp.sum(x32 * x32, axis=1),
            jnp.sum(e32 * e32, axis=1),
            jnp.sum(e32 * gain_own[None, :] * grad_norm, axis=1),
        ]
    )
    stats = jnp.pad(stats, (0, -stats.shape[0] % 1024)).reshape(-1, 128)
    stats = plane_sum(stats, f_size, t_size).reshape(-1)
    n_tok, n_frames = f_size * tok, f_size * block_frames
    inv_tok = lax.rsqrt(stats[:n_tok] / full_width + norm_eps)
    inv_frame = lax.rsqrt(stats[n_tok : n_tok + n_frames] / full_width + norm_eps)
    dots = inv_frame * stats[n_tok + n_frames : n_tok + 2 * n_frames]
    frame_grad = (
        (inv_frame[:, None] * gain_own[None, :]) * grad_norm
        - e32 * (inv_frame * inv_frame * dots / full_width)[:, None]
    ).astype(jnp.bfloat16)
    frame_grad = lax.all_gather(frame_grad, "fsdp", axis=1, tiled=True)
    projector_grad = product(frames_all.T, frame_grad)

    normed = (x32 * inv_tok[:, None] * gain_own[None, :]).astype(jnp.bfloat16)
    low_part = jnp.dot(normed, down_own, preferred_element_type=jnp.float32)
    value_part = jnp.dot(normed, frozen_own, preferred_element_type=jnp.float32)
    value_part = value_part + adapter_scale * jnp.dot(
        low_part.astype(jnp.bfloat16), up_full, preferred_element_type=jnp.float32
    )
    value_part = value_part.astype(jnp.bfloat16).reshape(f_size * tok, t_size, v_shard)
    low_send = jnp.broadcast_to(
        low_part.astype(jnp.bfloat16)[:, None, :], (f_size * tok, t_size, rank)
    )
    sent = jnp.concatenate([value_part, low_send], axis=2).transpose(1, 0, 2)
    got = lax.all_to_all(sent, "tp", split_axis=0, concat_axis=0, tiled=True)
    pair = jnp.sum(got.astype(jnp.float32), axis=0).astype(jnp.bfloat16)
    pair = pair.reshape(f_size, tok, v_shard + rank)
    got = lax.all_to_all(pair, "fsdp", split_axis=0, concat_axis=0, tiled=True)
    total = jnp.sum(got.astype(jnp.float32), axis=0)
    value_output = total[:, :v_shard].astype(jnp.bfloat16)
    low_half = total[:, v_shard:].astype(jnp.bfloat16)

    up_part = adapter_scale * contract_leading(low_half, grad_out)
    down_part = contract_leading(normed, lora_plane)
    both_parts = jnp.concatenate([down_part.reshape(-1, 128), up_part.reshape(-1, 128)], axis=0)
    summed = line_sum(both_parts, lax.axis_size("grp"), 4, 3)
    (gathered,) = fsdp_gather((summed.astype(jnp.bfloat16),), f_size, 4)
    gathered = gathered.astype(jnp.float32)
    split = cols * rank // 128
    down_map_gradient = gathered[:, :split].reshape(width, rank)
    up_map_gradient = jnp.sum(gathered[:, split:], axis=0).reshape(rank, v_shard)
    return (value_output, projector_grad, down_map_gradient, up_map_gradient)


def solution(mesh):
    in_specs = (
        P("fsdp", "grp"),
        P("grp", "tp"),
        P(("grp", "fsdp"), "tp"),
        P(),
        P("fsdp", "tp"),
        P("fsdp", None),
        P(None, "tp"),
        P("fsdp", None, None),
        P("fsdp", None, None),
        P(("grp", "fsdp")),
        P(),
        P(("grp", "fsdp"), "tp"),
    )
    out_specs = (P(("grp", "fsdp"), "tp"), P("grp", "tp"), P("tp", None), P(None, "tp"))
    return jax.shard_map(shards, mesh=mesh, in_specs=in_specs, out_specs=out_specs, check_vma=False)
```
